16 devices in a mesh: dp: 2 (over y, z), tp: 8 (over x, core).
Axes of the slice: x: 4, y: 2, z: 1, core: 2. Of those that a mesh axis runs over, the one named last changes fastest.
The devices are a block of a 4x4x8 slice.
Arguments:
- x_chunk: bfloat16 [8, 512, 4096], P('dp', 'tp'), parts along dimension 0
- prefix_len: int32 [8], P('dp'), parts along dimension 0
- k_cache: bfloat16 [8, 4096, 32, 128], P('dp', None, 'tp'), parts along dimension 0
- v_cache: bfloat16 [8, 4096, 32, 128], P('dp', None, 'tp'), parts along dimension 0
- ln1_gain: bfloat16 [4096], replicated
- ln1_bias: bfloat16 [4096], replicated
- w_qkv: bfloat16 [4096, 12288], P(None, 'tp')
- b_qkv: bfloat16 [12288], P('tp')
- w_out: bfloat16 [4096, 4096], P('tp')
- b_out: bfloat16 [4096], replicated
- ln2_gain: bfloat16 [4096], replicated
- ln2_bias: bfloat16 [4096], replicated
- w_up: bfloat16 [4096, 16384], P(None, 'tp')
- b_up: bfloat16 [16384], P('tp')
- w_down: bfloat16 [16384, 4096], P('tp')
- b_down: bfloat16 [4096], replicated
Outputs:
- output 1: bfloat16 [8, 512, 4096], P('dp', 'tp'), parts along dimension 0
- output 2: bfloat16 [8, 4096, 32, 128], P('dp', None, 'tp'), parts along dimension 0
- output 3: bfloat16 [8, 4096, 32, 128], P('dp', None, 'tp'), parts along dimension 0
There are 2 independent parts. The reference program is written for one: setup_inputs(seed, part) draws one part's arguments, and reference() takes and returns one part's arrays. A program takes and returns all parts, laid end to end along the dimension named above; an argument that names none is the same for every part.
All inputs are finite; a program needn't handle non-finite values.
Results may differ from the reference program's by a relative error of at most 0.0132093.
Values are sent between devices in bfloat16 or wider.
A program may use at most 768 MiB of HBM per device.

```python
import jax
import jax.numpy as jnp
from jax import lax

BATCH_SEQS = 4
CHUNK_LEN = 512
CACHE_LEN = 4096
D_MODEL = 4096
NUM_HEADS = 32
HEAD_DIM = 128
FF_DIM = 4 * D_MODEL
LN_EPS = 1e-5


def setup_inputs(seed: int = 0, part: int = 0) -> dict:
    part_keys = jax.random.split(jax.random.fold_in(jax.random.key(seed), part), 5)
    shared_keys = jax.random.split(jax.random.key(seed + 7919), 12)
    max_start = CACHE_LEN - CHUNK_LEN
    starts = jax.random.randint(part_keys[1], (BATCH_SEQS,), 0, max_start + 1)
    longest = jax.random.randint(part_keys[2], (), 0, BATCH_SEQS)
    prefix_len = jnp.where(jnp.arange(BATCH_SEQS) == longest, max_start, starts).astype(jnp.int32)
    cache_shape = (BATCH_SEQS, CACHE_LEN, NUM_HEADS, HEAD_DIM)
    vec_shape = (D_MODEL,)
    d_scale = D_MODEL ** -0.5

    def normal_draw(key_in, shape_in, std_dev):
        return (std_dev * jax.random.normal(key_in, shape_in, jnp.float32)).astype(jnp.bfloat16)

    def gain_draw(key_in):
        return (1.0 + 0.25 * jax.random.normal(key_in, vec_shape, jnp.float32)).astype(jnp.bfloat16)

    return {
        'x_chunk': normal_draw(part_keys[0], (BATCH_SEQS, CHUNK_LEN, D_MODEL), 1.0),
        'prefix_len': prefix_len,
        'k_cache': normal_draw(part_keys[3], cache_shape, 1.0),
        'v_cache': normal_draw(part_keys[4], cache_shape, 1.0),
        'ln1_gain': gain_draw(shared_keys[0]),
        'ln1_bias': normal_draw(shared_keys[1], vec_shape, 0.25),
        'w_qkv': normal_draw(shared_keys[2], (D_MODEL, 3 * D_MODEL), d_scale),
        'b_qkv': normal_draw(shared_keys[3], (3 * D_MODEL,), 0.25),
        'w_out': normal_draw(shared_keys[4], (D_MODEL, D_MODEL), d_scale),
        'b_out': normal_draw(shared_keys[5], vec_shape, 0.25),
        'ln2_gain': gain_draw(shared_keys[6]),
        'ln2_bias': normal_draw(shared_keys[7], vec_shape, 0.25),
        'w_up': normal_draw(shared_keys[8], (D_MODEL, FF_DIM), d_scale),
        'b_up': normal_draw(shared_keys[9], (FF_DIM,), 0.25),
        'w_down': normal_draw(shared_keys[10], (FF_DIM, D_MODEL), FF_DIM ** -0.5),
        'b_down': normal_draw(shared_keys[11], vec_shape, 0.25),
    }


def layer_norm(tok_rows, ln_gain, ln_bias):
    rows_f32 = tok_rows.astype(jnp.float32)
    row_mean = jnp.mean(rows_f32, axis=-1, keepdims=True)
    centered = rows_f32 - row_mean
    row_var = jnp.mean(centered * centered, axis=-1, keepdims=True)
    normed = centered * lax.rsqrt(row_var + LN_EPS)
    return (normed * ln_gain.astype(jnp.float32) + ln_bias.astype(jnp.float32)).astype(jnp.bfloat16)


def write_rows(cache_seq, new_rows, start_pos):
    zero_idx = jnp.zeros_like(start_pos)
    return lax.dynamic_update_slice(cache_seq, new_rows, (start_pos, zero_idx, zero_idx))


def attend_one(operands):
    queries, keys_all, values_all, start_pos = operands
    scores = jnp.einsum('chd,thd->hct', queries.astype(jnp.float32), keys_all.astype(jnp.float32)) * (HEAD_DIM ** -0.5)
    slopes = jnp.exp2(-8.0 * (jnp.arange(NUM_HEADS) + 1).astype(jnp.float32) / NUM_HEADS)
    query_pos = start_pos + jnp.arange(CHUNK_LEN)
    rel_pos = (jnp.arange(CACHE_LEN)[None, :] - query_pos[:, None]).astype(jnp.float32)
    scores = scores + slopes[:, None, None] * rel_pos[None]
    scores = jnp.where((rel_pos <= 0.0)[None], scores, -1e30)
    attn_probs = jax.nn.softmax(scores, axis=-1).astype(jnp.bfloat16)
    context = jnp.einsum('hct,thd->chd', attn_probs.astype(jnp.float32), values_all.astype(jnp.float32))
    return context.astype(jnp.bfloat16).reshape(CHUNK_LEN, D_MODEL)


def reference(x_chunk, prefix_len, k_cache, v_cache, ln1_gain, ln1_bias, w_qkv, b_qkv, w_out, b_out, ln2_gain, ln2_bias, w_up, b_up, w_down, b_down):
    tok_rows = x_chunk.reshape(BATCH_SEQS * CHUNK_LEN, D_MODEL)
    normed = layer_norm(tok_rows, ln1_gain, ln1_bias)
    qkv_proj = jnp.dot(normed, w_qkv, preferred_element_type=jnp.float32) + b_qkv.astype(jnp.float32)
    qkv_heads = qkv_proj.astype(jnp.bfloat16).reshape(BATCH_SEQS, CHUNK_LEN, NUM_HEADS, 3, HEAD_DIM)
    k_upd = jax.vmap(write_rows)(k_cache, qkv_heads[:, :, :, 1], prefix_len)
    v_upd = jax.vmap(write_rows)(v_cache, qkv_heads[:, :, :, 2], prefix_len)
    context = lax.map(attend_one, (qkv_heads[:, :, :, 0], k_upd, v_upd, prefix_len))
    context = context.reshape(BATCH_SEQS * CHUNK_LEN, D_MODEL)
    attn_out = jnp.dot(context, w_out, preferred_element_type=jnp.float32)
    residual = (tok_rows.astype(jnp.float32) + attn_out + b_out.astype(jnp.float32)).astype(jnp.bfloat16)
    normed2 = layer_norm(residual, ln2_gain, ln2_bias)
    up_pre = jnp.dot(normed2, w_up, preferred_element_type=jnp.float32) + b_up.astype(jnp.float32)
    up_act = jax.nn.gelu(up_pre, approximate=True).astype(jnp.bfloat16)
    down_out = jnp.dot(up_act, w_down, preferred_element_type=jnp.float32)
    x_out = (residual.astype(jnp.float32) + down_out + b_down.astype(jnp.float32)).astype(jnp.bfloat16)
    return x_out.reshape(BATCH_SEQS, CHUNK_LEN, D_MODEL), k_upd, v_upd
```

```python
import functools

import jax
import jax.numpy as jnp
from jax import lax
from jax.experimental import pallas as pl
from jax.experimental.pallas import tpu as pltpu
from jax.sharding import PartitionSpec as P

LN_EPS = 1e-5
LOG2E = 1.4426950408889634
NEG = -1e30
KEY_BLOCK = 512
QUERY_SUB = 128
SPLITS = (2, 2)


def layer_norm(tok_rows, ln_gain, ln_bias):
    rows_f32 = tok_rows.astype(jnp.float32)
    row_mean = jnp.mean(rows_f32, axis=-1, keepdims=True)
    centered = rows_f32 - row_mean
    row_var = jnp.mean(centered * centered, axis=-1, keepdims=True)
    normed = centered * lax.rsqrt(row_var + LN_EPS)
    return (normed * ln_gain.astype(jnp.float32) + ln_bias.astype(jnp.float32)).astype(jnp.bfloat16)


def attend_kernel(seq0, heads, heads_all, plen_ref, head0_ref, qkv_ref, k_ref, v_ref, k_old, v_old, ctx_ref, ko_ref, vo_ref,
                  acc, row_max, row_sum, kf, vf, knew, vnew, q_t, sems):
    del k_old, v_old
    seq = pl.program_id(0)
    kb = pl.program_id(1)
    n_kb = pl.num_programs(1) - 1
    tb, hd = k_ref.shape[1] // heads, k_ref.shape[2]
    chunk = qkv_ref.shape[1]
    plen = plen_ref[seq + seq0]
    base = kb * tb
    scale = (hd ** -0.5) * LOG2E
    k_put = pltpu.make_async_copy(knew, ko_ref.at[seq + seq0, pl.ds(plen, chunk)], sems.at[0])
    v_put = pltpu.make_async_copy(vnew, vo_ref.at[seq + seq0, pl.ds(plen, chunk)], sems.at[1])

    @pl.when(kb == 0)
    def _():
        acc[...] = jnp.zeros_like(acc)
        row_max[...] = jnp.full_like(row_max, NEG)
        row_sum[...] = jnp.zeros_like(row_sum)
        for h in range(heads):
            c = h * 3 * hd
            q_t[h] = qkv_ref[0, :, c:c + hd].T
            kf[pl.ds(h, chunk, stride=heads), :] = qkv_ref[0, :, c + hd:c + 2 * hd].astype(jnp.float32)
            vf[pl.ds(h, chunk, stride=heads), :] = qkv_ref[0, :, c + 2 * hd:c + 3 * hd].astype(jnp.float32)
        knew[...] = kf[...].reshape(chunk, heads, hd).astype(jnp.bfloat16)
        vnew[...] = vf[...].reshape(chunk, heads, hd).astype(jnp.bfloat16)
        k_put.start()
        v_put.start()

    def slope(h):
        head_id = (head0_ref[0] + h + 1).astype(jnp.float32)
        return jnp.exp2(jnp.full((1, 1), -8.0 / heads_all, jnp.float32) * head_id) * LOG2E

    def step(h, keys, vals, bias_pos, mask):
        bias = slope(h) * bias_pos
        for c0 in range(0, chunk, QUERY_SUB):
            cols = slice(c0, c0 + QUERY_SUB)
            s = lax.dot_general(keys, q_t[h, :, cols], (((1,), (0,)), ((), ())), preferred_element_type=jnp.float32)
            s = s * scale + bias
            if mask is not None:
                s = jnp.where(mask if mask.shape[1] == 1 else mask[:, cols], s, NEG)
            m_old = row_max[h:h + 1, cols]
            m_new = jnp.maximum(m_old, jnp.max(s, axis=0, keepdims=True))
            alpha = jnp.exp2(m_old - m_new)
            p = jnp.exp2(s - m_new)
            row_sum[h:h + 1, cols] = row_sum[h:h + 1, cols] * alpha + jnp.sum(p, axis=0, keepdims=True)
            row_max[h:h + 1, cols] = m_new
            pv = lax.dot_general(vals, p.astype(jnp.bfloat16), (((0,), (0,)), ((), ())), preferred_element_type=jnp.float32)
            acc[h, :, cols] = acc[h, :, cols] * alpha + pv

    def prefix(masked):
        kf[...] = k_ref[0].astype(jnp.float32)
        vf[...] = v_ref[0].astype(jnp.float32)
        slot = base + lax.broadcasted_iota(jnp.int32, (tb, 1), 0)
        bias_pos = (slot - (plen + chunk - 1)).astype(jnp.float32)
        mask = (slot < plen) if masked else None
        for h in range(heads):
            keys = kf[pl.ds(h, tb, stride=heads), :].astype(jnp.bfloat16)
            vals = vf[pl.ds(h, tb, stride=heads), :].astype(jnp.bfloat16)
            step(h, keys, vals, bias_pos, mask)

    @pl.when((kb < n_kb) & (base + tb <= plen))
    def _():
        prefix(False)

    @pl.when((kb < n_kb) & (base < plen) & (base + tb > plen))
    def _():
        prefix(True)

    @pl.when(kb == n_kb)
    def _():
        key_i = lax.broadcasted_iota(jnp.int32, (chunk, chunk), 0)
        qry_i = lax.broadcasted_iota(jnp.int32, (chunk, chunk), 1)
        mask = key_i <= qry_i
        bias_pos = (lax.broadcasted_iota(jnp.int32, (chunk, 1), 0) - (chunk - 1)).astype(jnp.float32)
        for h in range(heads):
            c = h * 3 * hd
            keys = qkv_ref[0, :, c + hd:c + 2 * hd]
            vals = qkv_ref[0, :, c + 2 * hd:c + 3 * hd]
            step(h, keys, vals, bias_pos, mask)
            out = acc[h] / row_sum[h:h + 1, :]
            ctx_ref[0, :, h * hd:(h + 1) * hd] = out.T.astype(jnp.bfloat16)
        k_put.wait()
        v_put.wait()


def attend(qkv, plen, head0, k_cache, v_cache, k_out, v_out, seq0, heads_all):
    n_seq, chunk, _ = qkv.shape
    all_seq, cache_len, heads, hd = k_cache.shape
    tb = KEY_BLOCK
    n_kb = cache_len // tb

    def cache_block(b, k, plen_ref, _):
        need = (plen_ref[b + seq0] + tb - 1) // tb
        return b + seq0, jnp.minimum(k, jnp.maximum(need - 1, 0)), 0

    cache_spec = pl.BlockSpec((1, tb * heads, hd), cache_block)
    any_spec = pl.BlockSpec(memory_space=pl.ANY)
    rows = (all_seq, cache_len * heads, hd)
    grid_spec = pltpu.PrefetchScalarGridSpec(
        num_scalar_prefetch=2, grid=(n_seq, n_kb + 1),
        in_specs=[pl.BlockSpec((1, chunk, heads * 3 * hd), lambda b, k, *_: (b, 0, 0)), cache_spec, cache_spec, any_spec, any_spec],
        out_specs=[pl.BlockSpec((1, chunk, heads * hd), lambda b, k, *_: (b, 0, 0)), any_spec, any_spec],
        scratch_shapes=[pltpu.VMEM((heads, hd, chunk), jnp.float32), pltpu.VMEM((heads, chunk), jnp.float32),
                        pltpu.VMEM((heads, chunk), jnp.float32), pltpu.VMEM((tb * heads, hd), jnp.float32),
                        pltpu.VMEM((tb * heads, hd), jnp.float32), pltpu.VMEM((chunk, heads, hd), jnp.bfloat16),
                        pltpu.VMEM((chunk, heads, hd), jnp.bfloat16), pltpu.VMEM((heads, hd, chunk), jnp.bfloat16),
                        pltpu.SemaphoreType.DMA((2,))])
    return pl.pallas_call(
        functools.partial(attend_kernel, seq0, heads, heads_all), grid_spec=grid_spec,
        out_shape=[jax.ShapeDtypeStruct((n_seq, chunk, heads * hd), jnp.bfloat16),
                   jax.ShapeDtypeStruct(k_cache.shape, k_cache.dtype), jax.ShapeDtypeStruct(v_cache.shape, v_cache.dtype)],
        input_output_aliases={5: 1, 6: 2},
        cost_estimate=pl.CostEstimate(flops=4 * n_seq * heads * chunk * cache_len * hd * 3, transcendentals=0,
                                      bytes_accessed=8 * n_seq * cache_len * heads * hd),
        compiler_params=pltpu.CompilerParams(vmem_limit_bytes=60 * 1024 * 1024,
                                             dimension_semantics=("arbitrary", "arbitrary")),
    )(plen, head0, qkv, k_cache.reshape(rows), v_cache.reshape(rows), k_out, v_out)


def solution(mesh):
    tp_size = mesh.shape['tp']

    def local_layer(x_local, prefix_len, k_cache, v_cache, ln1_gain, ln1_bias, w_qkv, b_qkv, w_out, b_out, ln2_gain, ln2_bias, w_up, b_up, w_down, b_down):
        heads_loc = k_cache.shape[2]
        heads_all = heads_loc * tp_size
        head0 = (lax.axis_index('tp') * heads_loc).astype(jnp.int32).reshape(1)
        k_out, v_out = k_cache, v_cache
        bounds = [sum(SPLITS[:i]) for i in range(len(SPLITS) + 1)]
        x_parts = [x_local[lo:hi] for lo, hi in zip(bounds, bounds[1:])]
        gathered = []
        for i, x_part in enumerate(x_parts):
            if i > 0:
                x_part, normed = lax.optimization_barrier((x_part, normed))
                gathered.append(lax.all_gather(normed, 'tp', axis=1, tiled=True))
            normed = layer_norm(x_part, ln1_gain, ln1_bias)
        gathered.append(lax.all_gather(normed, 'tp', axis=1, tiled=True))
        attn_parts = []
        for i, g in enumerate(gathered):
            if i > 0:
                g, attn_parts[-1] = lax.optimization_barrier((g, attn_parts[-1]))
            qkv = (jnp.einsum('bcd,de->bce', g, w_qkv, preferred_element_type=jnp.float32) + b_qkv.astype(jnp.float32)).astype(jnp.bfloat16)
            context, k_out, v_out = attend(qkv, prefix_len, head0, k_cache, v_cache, k_out, v_out, bounds[i], heads_all)
            attn_parts.append(jnp.einsum('bce,ed->bcd', context, w_out, preferred_element_type=jnp.float32).astype(jnp.bfloat16))
        residuals, gathered2 = [], []
        for i, attn_part in enumerate(attn_parts):
            attn_sum = lax.psum_scatter(attn_part, 'tp', scatter_dimension=1, tiled=True)
            if i > 0:
                attn_sum, normed2 = lax.optimization_barrier((attn_sum, normed2))
                gathered2.append(lax.all_gather(normed2, 'tp', axis=1, tiled=True))
            residual = (x_parts[i].astype(jnp.float32) + attn_sum.astype(jnp.float32) + b_out.astype(jnp.float32)).astype(jnp.bfloat16)
            normed2 = layer_norm(residual, ln2_gain, ln2_bias)
            residuals.append(residual)
        gathered2.append(lax.all_gather(normed2, 'tp', axis=1, tiled=True))
        outs = []
        for i, g in enumerate(gathered2):
            up_pre = jnp.einsum('bcd,df->bcf', g, w_up, preferred_element_type=jnp.float32) + b_up.astype(jnp.float32)
            up_act = jax.nn.gelu(up_pre, approximate=True).astype(jnp.bfloat16)
            down_part = jnp.einsum('bcf,fd->bcd', up_act, w_down, preferred_element_type=jnp.float32).astype(jnp.bfloat16)
            down_sum = lax.psum_scatter(down_part, 'tp', scatter_dimension=1, tiled=True)
            if i > 0:
                down_sum, outs[-1] = lax.optimization_barrier((down_sum, outs[-1]))
            outs.append((residuals[i].astype(jnp.float32) + down_sum.astype(jnp.float32) + b_down.astype(jnp.float32)).astype(jnp.bfloat16))
        return jnp.concatenate(outs, axis=0), k_out, v_out

    tok_spec = P('dp', 'tp', None)
    cache_spec = P('dp', None, 'tp', None)
    replicated = P()
    in_specs = (tok_spec, P('dp'), cache_spec, cache_spec, replicated, replicated, P(None, 'tp'), P('tp'), P('tp', None), replicated, replicated, replicated, P(None, 'tp'), P('tp'), P('tp', None), replicated)
    return jax.shard_map(local_layer, mesh=mesh, in_specs=in_specs, out_specs=(tok_spec, cache_spec, cache_spec), check_vma=False)
```

```python
import functools

import jax
import jax.numpy as jnp
from jax import lax
from jax.experimental import pallas as pl
from jax.experimental.pallas import tpu as pltpu
from jax.sharding import PartitionSpec as P

LN_EPS = 1e-5
LOG2E = 1.4426950408889634
NEG = -1e30
KEY_BLOCK = 512
QUERY_SUB = 128
SPLITS = (2, 2)


def layer_norm(tok_rows, ln_gain, ln_bias):
    rows_f32 = tok_rows.astype(jnp.float32)
    row_mean = jnp.mean(rows_f32, axis=-1, keepdims=True)
    centered = rows_f32 - row_mean
    row_var = jnp.mean(centered * centered, axis=-1, keepdims=True)
    normed = centered * lax.rsqrt(row_var + LN_EPS)
    return (normed * ln_gain.astype(jnp.float32) + ln_bias.astype(jnp.float32)).astype(jnp.bfloat16)


def attend_kernel(seq0, heads, heads_all, plen_ref, head0_ref, qkv_ref, k_ref, v_ref, k_old, v_old, ctx_ref, ko_ref, vo_ref,
                  acc, row_max, row_sum, kf, vf, knew, vnew, q_t, sems):
    del k_old, v_old
    seq = pl.program_id(0)
    kb = pl.program_id(1)
    n_kb = pl.num_programs(1) - 1
    tb, hd = k_ref.shape[1] // heads, k_ref.shape[2]
    chunk = qkv_ref.shape[1]
    plen = plen_ref[seq + seq0]
    base = kb * tb
    scale = (hd ** -0.5) * LOG2E
    k_put = pltpu.make_async_copy(knew, ko_ref.at[seq + seq0, pl.ds(plen, chunk)], sems.at[0])
    v_put = pltpu.make_async_copy(vnew, vo_ref.at[seq + seq0, pl.ds(plen, chunk)], sems.at[1])

    @pl.when(kb == 0)
    def _():
        acc[...] = jnp.zeros_like(acc)
        row_max[...] = jnp.full_like(row_max, NEG)
        row_sum[...] = jnp.zeros_like(row_sum)
        for h in range(heads):
            c = h * 3 * hd
            q_t[h] = qkv_ref[0, :, c:c + hd].T
            kf[pl.ds(h, chunk, stride=heads), :] = qkv_ref[0, :, c + hd:c + 2 * hd].astype(jnp.float32)
            vf[pl.ds(h, chunk, stride=heads), :] = qkv_ref[0, :, c + 2 * hd:c + 3 * hd].astype(jnp.float32)
        knew[...] = kf[...].reshape(chunk, heads, hd).astype(jnp.bfloat16)
        vnew[...] = vf[...].reshape(chunk, heads, hd).astype(jnp.bfloat16)
        k_put.start()
        v_put.start()

    def slope(h):
        head_id = (head0_ref[0] + h + 1).astype(jnp.float32)
        return jnp.exp2(jnp.full((1, 1), -8.0 / heads_all, jnp.float32) * head_id) * LOG2E

    def step(h, keys, vals, bias_pos, mask):
        bias = slope(h) * bias_pos
        for c0 in range(0, chunk, QUERY_SUB):
            cols = slice(c0, c0 + QUERY_SUB)
            s = lax.dot_general(keys, q_t[h, :, cols], (((1,), (0,)), ((), ())), preferred_element_type=jnp.float32)
            s = s * scale + bias
            if mask is not None:
                s = jnp.where(mask if mask.shape[1] == 1 else mask[:, cols], s, NEG)
            m_old = row_max[h:h + 1, cols]
            m_new = jnp.maximum(m_old, jnp.max(s, axis=0, keepdims=True))
            alpha = jnp.exp2(m_old - m_new)
            p = jnp.exp2(s - m_new)
            row_sum[h:h + 1, cols] = row_sum[h:h + 1, cols] * alpha + jnp.sum(p, axis=0, keepdims=True)
            row_max[h:h + 1, cols] = m_new
            pv = lax.dot_general(vals, p.astype(jnp.bfloat16), (((0,), (0,)), ((), ())), preferred_element_type=jnp.float32)
            acc[h, :, cols] = acc[h, :, cols] * alpha + pv

    def prefix(masked):
        kf[...] = k_ref[0].astype(jnp.float32)
        vf[...] = v_ref[0].astype(jnp.float32)
        slot = base + lax.broadcasted_iota(jnp.int32, (tb, 1), 0)
        bias_pos = (slot - (plen + chunk - 1)).astype(jnp.float32)
        mask = (slot < plen) if masked else None
        for h in range(heads):
            keys = kf[pl.ds(h, tb, stride=heads), :].astype(jnp.bfloat16)
            vals = vf[pl.ds(h, tb, stride=heads), :].astype(jnp.bfloat16)
            step(h, keys, vals, bias_pos, mask)

    @pl.when((kb < n_kb) & (base + tb <= plen))
    def _():
        prefix(False)

    @pl.when((kb < n_kb) & (base < plen) & (base + tb > plen))
    def _():
        prefix(True)

    @pl.when(kb == n_kb)
    def _():
        key_i = lax.broadcasted_iota(jnp.int32, (chunk, chunk), 0)
        qry_i = lax.broadcasted_iota(jnp.int32, (chunk, chunk), 1)
        mask = key_i <= qry_i
        bias_pos = (lax.broadcasted_iota(jnp.int32, (chunk, 1), 0) - (chunk - 1)).astype(jnp.float32)
        for h in range(heads):
            c = h * 3 * hd
            keys = qkv_ref[0, :, c + hd:c + 2 * hd]
            vals = qkv_ref[0, :, c + 2 * hd:c + 3 * hd]
            step(h, keys, vals, bias_pos, mask)
            out = acc[h] / row_sum[h:h + 1, :]
            ctx_ref[0, :, h * hd:(h + 1) * hd] = out.T.astype(jnp.bfloat16)
        k_put.wait()
        v_put.wait()


def attend(qkv, plen, head0, k_cache, v_cache, k_out, v_out, seq0, heads_all):
    n_seq, chunk, _ = qkv.shape
    all_seq, cache_len, heads, hd = k_cache.shape
    tb = KEY_BLOCK
    n_kb = cache_len // tb

    def cache_block(b, k, plen_ref, _):
        need = (plen_ref[b + seq0] + tb - 1) // tb
        return b + seq0, jnp.minimum(k, jnp.maximum(need - 1, 0)), 0

    cache_spec = pl.BlockSpec((1, tb * heads, hd), cache_block)
    any_spec = pl.BlockSpec(memory_space=pl.ANY)
    rows = (all_seq, cache_len * heads, hd)
    grid_spec = pltpu.PrefetchScalarGridSpec(
        num_scalar_prefetch=2, grid=(n_seq, n_kb + 1),
        in_specs=[pl.BlockSpec((1, chunk, heads * 3 * hd), lambda b, k, *_: (b, 0, 0)), cache_spec, cache_spec, any_spec, any_spec],
        out_specs=[pl.BlockSpec((1, chunk, heads * hd), lambda b, k, *_: (b, 0, 0)), any_spec, any_spec],
        scratch_shapes=[pltpu.VMEM((heads, hd, chunk), jnp.float32), pltpu.VMEM((heads, chunk), jnp.float32),
                        pltpu.VMEM((heads, chunk), jnp.float32), pltpu.VMEM((tb * heads, hd), jnp.float32),
                        pltpu.VMEM((tb * heads, hd), jnp.float32), pltpu.VMEM((chunk, heads, hd), jnp.bfloat16),
                        pltpu.VMEM((chunk, heads, hd), jnp.bfloat16), pltpu.VMEM((heads, hd, chunk), jnp.bfloat16),
                        pltpu.SemaphoreType.DMA((2,))])
    return pl.pallas_call(
        functools.partial(attend_kernel, seq0, heads, heads_all), grid_spec=grid_spec,
        out_shape=[jax.ShapeDtypeStruct((n_seq, chunk, heads * hd), jnp.bfloat16),
                   jax.ShapeDtypeStruct(k_cache.shape, k_cache.dtype), jax.ShapeDtypeStruct(v_cache.shape, v_cache.dtype)],
        input_output_aliases={5: 1, 6: 2},
        cost_estimate=pl.CostEstimate(flops=4 * n_seq * heads * chunk * cache_len * hd * 3, transcendentals=0,
                                      bytes_accessed=8 * n_seq * cache_len * heads * hd),
        compiler_params=pltpu.CompilerParams(vmem_limit_bytes=60 * 1024 * 1024,
                                             dimension_semantics=("arbitrary", "arbitrary")),
    )(plen, head0, qkv, k_cache.reshape(rows), v_cache.reshape(rows), k_out, v_out)


def copy_kernel(src_ref, dst_ref):
    dst_ref[...] = src_ref[...]


def copy_cache(cache):
    seqs, cache_len, heads, hd = cache.shape
    rows = cache_len * heads
    spec = pl.BlockSpec((1, rows // 4, hd), lambda b, k: (b, k, 0))
    out = pl.pallas_call(
        copy_kernel, grid=(seqs, 4), in_specs=[spec], out_specs=spec,
        out_shape=jax.ShapeDtypeStruct((seqs, rows, hd), cache.dtype),
        cost_estimate=pl.CostEstimate(flops=seqs * rows * hd * 1000, transcendentals=0, bytes_accessed=4 * seqs * rows * hd),
        compiler_params=pltpu.CompilerParams(vmem_limit_bytes=60 * 1024 * 1024),
    )(cache.reshape(seqs, rows, hd))
    return out.reshape(cache.shape)


def solution(mesh):
    tp_size = mesh.shape['tp']

    def local_layer(x_local, prefix_len, k_cache, v_cache, ln1_gain, ln1_bias, w_qkv, b_qkv, w_out, b_out, ln2_gain, ln2_bias, w_up, b_up, w_down, b_down):
        heads_loc = k_cache.shape[2]
        heads_all = heads_loc * tp_size
        head0 = (lax.axis_index('tp') * heads_loc).astype(jnp.int32).reshape(1)
        core = lax.rem(lax.axis_index('tp'), 2)
        chips = tp_size // 2
        groups = [[chip * 2 + c for chip in range(chips)] for c in range(2)]
        swap = [(i, i ^ 1) for i in range(tp_size)]
        barrier = lax.optimization_barrier
        half = SPLITS[0]
        x_parts = [x_local[None, :half], x_local[None, half:]]

        def gather(rows):
            return lax.all_gather(rows, 'tp', axis=0, tiled=True, axis_index_groups=groups)

        def scatter(rows):
            return lax.psum_scatter(rows, 'tp', scatter_dimension=0, tiled=True, axis_index_groups=groups)

        def to_partner(rows):
            return lax.ppermute(rows, 'tp', swap)

        def matmul(rows, weight):
            return jnp.einsum('xbtc,cd->xbtd', rows, weight, preferred_element_type=jnp.float32)

        def chip_sum(for_partner, own, weight):
            received = to_partner(matmul(for_partner, weight).astype(jnp.bfloat16))
            return (matmul(own, weight) + received.astype(jnp.float32)).astype(jnp.bfloat16)

        def project_qkv(g):
            own, partner = [(matmul(rows, w_qkv) + b_qkv.astype(jnp.float32)).astype(jnp.bfloat16) for rows in (g, to_partner(g))]
            first = core == 0
            pair = jnp.stack([jnp.where(first, own, partner), jnp.where(first, partner, own)], axis=1)
            return jnp.transpose(pair, (2, 0, 1, 3, 4)).reshape(own.shape[1], -1, own.shape[-1])

        def project_out(context):
            pairs = context.reshape(context.shape[0], chips, 2, x_local.shape[1], context.shape[-1])
            own = lax.dynamic_index_in_dim(pairs, core, axis=2, keepdims=False)
            partner = lax.dynamic_index_in_dim(pairs, 1 - core, axis=2, keepdims=False)
            return chip_sum(jnp.swapaxes(partner, 0, 1), jnp.swapaxes(own, 0, 1), w_out)

        def add_bias(rows, total, bias):
            return (rows.astype(jnp.float32) + total.astype(jnp.float32) + bias.astype(jnp.float32)).astype(jnp.bfloat16)

        def mlp(g):
            own, partner = [
                jax.nn.gelu(matmul(rows, w_up) + b_up.astype(jnp.float32), approximate=True).astype(jnp.bfloat16)
                for rows in (g, to_partner(g))]
            return chip_sum(partner, own, w_down)

        norm_a = layer_norm(x_parts[0], ln1_gain, ln1_bias)
        x_b, norm_a = barrier((x_parts[1], norm_a))
        gath_a = gather(norm_a)
        gath_b = gather(layer_norm(x_b, ln1_gain, ln1_bias))
        k_out, v_out = copy_cache(k_cache), copy_cache(v_cache)
        gath_a, k_out, v_out = barrier((gath_a, k_out, v_out))
        ctx_a, k_out, v_out = attend(project_qkv(gath_a), prefix_len, head0, k_cache, v_cache, k_out, v_out, 0, heads_all)
        part_a = project_out(ctx_a)
        gath_b, part_a = barrier((gath_b, part_a))
        sum_a = scatter(part_a)
        ctx_b, k_out, v_out = attend(project_qkv(gath_b), prefix_len, head0, k_cache, v_cache, k_out, v_out, half, heads_all)
        res_a = add_bias(x_parts[0], sum_a, b_out)
        norm_a = layer_norm(res_a, ln2_gain, ln2_bias)
        ctx_b, norm_a = barrier((ctx_b, norm_a))
        gath_a = gather(norm_a)
        sum_b = scatter(project_out(ctx_b))
        down_a = mlp(gath_a)
        res_b = add_bias(x_parts[1], sum_b, b_out)
        gath_b = gather(layer_norm(res_b, ln2_gain, ln2_bias))
        gath_b, down_a = barrier((gath_b, down_a))
        tot_a = scatter(down_a)
        tot_b = scatter(mlp(gath_b))
        out_a = add_bias(res_a, tot_a, b_down)
        tot_b, out_a = barrier((tot_b, out_a))
        out_b = add_bias(res_b, tot_b, b_down)
        return jnp.concatenate([out_a, out_b], axis=1)[0], k_out, v_out

    tok_spec = P('dp', 'tp', None)
    cache_spec = P('dp', None, 'tp', None)
    replicated = P()
    in_specs = (tok_spec, P('dp'), cache_spec, cache_spec, replicated, replicated, P(None, 'tp'), P('tp'), P('tp', None), replicated, replicated, replicated, P(None, 'tp'), P('tp'), P('tp', None), replicated)
    return jax.shard_map(local_layer, mesh=mesh, in_specs=in_specs, out_specs=(tok_spec, cache_spec, cache_spec), check_vma=False)
```
